32 devices in a mesh: row: 16 (over z, x, core), col: 2 (over y).
Axes of the slice: x: 2, y: 2, z: 4, core: 2. Of those that a mesh axis runs over, the one named last changes fastest.
Arguments:
- tokens: bfloat16 [1024, 8192], P('row', 'col'), may hold values from -6 to 6
- norm_gain: bfloat16 [8192], P('col'), may hold values from 0.099609375 to 1.8984375
- gate_proj: bfloat16 [8192, 28672], P('col', 'row'), may hold values from -0.0625 to 0.0625
- up_proj: bfloat16 [8192, 28672], P('col', 'row'), may hold values from -0.0625 to 0.0625
- down_proj: bfloat16 [28672, 8192], P('row', 'col'), may hold values from -0.03125 to 0.03125
Outputs:
- mixed: bfloat16 [1024, 8192], P('row', 'col')
The draws below stay inside these ranges and needn't reach their ends.
All inputs are finite; a program needn't handle non-finite values.
Results may differ from the reference program's by a relative error of at most 0.015.
Values may be sent and summed in bfloat16 or wider, within the bound.
A program may use at most 128 MiB of HBM per device.

```python
import jax
import jax.numpy as jnp
from jax import lax

D = 8192
FF = 28672
TOKENS = 1024


def steps_of(own_key, extent, split, smallest, top_value):
    level = 1.0
    for position, blocks in split:
        draws = jax.random.uniform(jax.random.fold_in(jax.random.fold_in(own_key, 6), position), (blocks,), jnp.float32, smallest / len(split), top_value / len(split))
        level = level * jnp.repeat(jnp.exp(draws), extent[position] // blocks).reshape((-1,) + (1,) * (len(extent) - 1 - position))
    return level


def noise(stream_key, extent, width, limit, cuts=(), dtype=jnp.bfloat16):
    factor_of = steps_of(stream_key, extent, cuts, -0.22, 0.18) if cuts else 1.0
    array = jax.random.normal(stream_key, extent, jnp.float32) * width * factor_of
    return jnp.minimum(jnp.maximum(array, -limit), limit).astype(dtype)


def setup_inputs(seed: int = 0) -> dict:
    streams_of = jax.random.split(jax.random.key(seed), 6)
    tokens = noise(streams_of[0], (TOKENS, D), 1.0, 6.0, ((0, 16), (1, 2)))
    norm_gain = jnp.clip(1.0 + 0.18 * jax.random.normal(streams_of[1], (D,), jnp.float32), 0.099609375, 1.8984375).astype(jnp.bfloat16)
    gate_proj = noise(streams_of[2], (D, FF), D ** -0.5, 0.0625, ((0, 2), (1, 16)))
    up_proj = noise(streams_of[3], (D, FF), D ** -0.5, 0.0625, ((0, 2), (1, 16)))
    down_proj = noise(streams_of[4], (FF, D), FF ** -0.5, 0.03125, ((0, 16), (1, 2)))
    return {"tokens": tokens, "norm_gain": norm_gain, "gate_proj": gate_proj, "up_proj": up_proj, "down_proj": down_proj}


floor_term = 0.25

def reference(tokens, norm_gain, gate_proj, up_proj, down_proj):
    widened = tokens.astype(jnp.float32)
    square_sum = lax.optimization_barrier(jnp.sum(widened * widened, axis=1))
    row_scale = 1.0 / jnp.sqrt(square_sum / D + floor_term)
    scaled = (widened * norm_gain.astype(jnp.float32)[None, :]).astype(jnp.bfloat16)
    gate = row_scale[:, None] * jnp.dot(scaled, gate_proj, preferred_element_type=jnp.float32)
    up_value = row_scale[:, None] * jnp.dot(scaled, up_proj, preferred_element_type=jnp.float32)
    hidden = (jax.nn.silu(gate) * up_value).astype(jnp.bfloat16)
    mixed = widened + jnp.dot(hidden, down_proj, preferred_element_type=jnp.float32)
    return mixed.astype(jnp.bfloat16)
```

```python
import functools

import jax
import jax.numpy as jnp
from jax import lax
from jax.experimental import pallas as pl
from jax.experimental.pallas import tpu as pltpu
from jax.sharding import PartitionSpec as P

floor_term = 0.25
MESH = pl.DeviceIdType.MESH
BF = jnp.bfloat16
F32 = jnp.float32


def places(rows):
    n = rows // 2
    row, col = lax.axis_index("row"), lax.axis_index("col")
    core, chip = row % 2, row // 2
    z, x = chip // 2, chip % 2
    pos = z + x * (n - 1 - 2 * z)

    def at(p):
        p = (p + n) % n
        far = (2 * p) // n
        return ((1 - far) * 2 * p + far * (2 * (n - 1 - p) + 1)) * 2 + core

    right, left = (at(pos + 1), col), (at(pos - 1), col)
    return core, col, right, left, (row + 1 - 2 * core, col), (row, 1 - col)


def greet(partners):
    barrier = pltpu.get_barrier_semaphore()
    for device in partners:
        pl.semaphore_signal(barrier, inc=1, device_id=device, device_id_type=MESH)
    pl.semaphore_wait(barrier, len(partners))


def remote(src, dst, send, recv, device):
    return pltpu.make_async_remote_copy(
        src_ref=src, dst_ref=dst, send_sem=send, recv_sem=recv, device_id=device, device_id_type=MESH
    )


def first_kernel(rows, cols, tile, tok, gain, wg_hbm, wu_hbm, hid, wg, wu, x, pb, rv, sq, sq_in,
                 w_sem, sq_sem, ring_s, ring_r, sib_s, sib_r, y_s, y_r):
    n = rows // 2
    half, width = tok.shape[0] // 2, tok.shape[1]
    units = wg.shape[1]
    load_g = pltpu.make_async_copy(wg_hbm, wg, w_sem.at[0])
    load_u = pltpu.make_async_copy(wu_hbm, wu, w_sem.at[1])
    load_g.start()
    load_u.start()
    core, col, right, left, sibling, across = places(rows)
    wide = tok[...].astype(F32)
    sq[...] = jnp.broadcast_to(jnp.sum(wide * wide, axis=1, keepdims=True), sq.shape)
    greet((right, left, sibling, across))
    sums = remote(sq, sq_in, sq_sem.at[0], sq_sem.at[1], across)
    sums.start()
    sums.wait()
    total = sq[:, 0:1] + sq_in[:, 0:1]
    scale = 1.0 / jnp.sqrt(total / (width * cols) + floor_term)
    normed = (tok[...].astype(F32) * gain[...].astype(F32) * scale).astype(BF)
    x[0, 0, core] = normed[:half]
    x[0, 1, core] = normed[half:]

    def ring(s, d):
        return remote(x.at[s, d, core], x.at[s + 1, d, core], ring_s.at[s, d], ring_r.at[s, d], (right, left)[d])

    def sib(s, d):
        return remote(x.at[s, d, core], x.at[s, d, core], sib_s.at[s, d], sib_r.at[s, d], sibling)

    def swap(s, g):
        return remote(pb.at[s, g, 1 - col], rv.at[s, g], y_s.at[s, g], y_r.at[s, g], across)

    def product(s, g, w):
        @pl.loop(0, units // tile)
        def _(t):
            at = pl.ds(pl.multiple_of(t * tile, tile), tile)
            part = jnp.dot(x[s].reshape(4 * half, width), w[:, at], preferred_element_type=F32)
            pb[s, g, :, :, at] = part.astype(BF).reshape(2, 2 * half, tile)
        swap(s, g).start()

    def finish(s):
        swap(s, 0).wait_recv()
        swap(s, 1).wait_recv()

        @pl.loop(0, units // tile)
        def _(t):
            at = pl.ds(pl.multiple_of(t * tile, tile), tile)
            gate = pb[s, 0, col, :, at].astype(F32) + rv[s, 0, :, at].astype(F32)
            up = pb[s, 1, col, :, at].astype(F32) + rv[s, 1, :, at].astype(F32)
            hid[s, :, at] = (gate / (1.0 + jnp.exp(-gate)) * up).astype(BF)

    @pl.loop(0, n)
    def _(s):
        @pl.when(s > 0)
        def _():
            ring(s - 1, 0).wait_recv()
            ring(s - 1, 1).wait_recv()

        @pl.when(s < n - 1)
        def _():
            ring(s, 0).start()
            ring(s, 1).start()

        sib(s, 0).start()
        sib(s, 1).start()
        sib(s, 0).wait_recv()
        sib(s, 1).wait_recv()

        @pl.when(s == 0)
        def _():
            load_g.wait()

        product(s, 0, wg)

        @pl.when(s == 0)
        def _():
            load_u.wait()

        product(s, 1, wu)

        @pl.when(s > 1)
        def _():
            finish(s - 2)

    @pl.loop(n - 2, n)
    def _(s):
        finish(s)

    @pl.loop(0, n)
    def _(s):
        for d in range(2):
            sib(s, d).wait_send()
            swap(s, d).wait_send()

        @pl.when(s < n - 1)
        def _():
            ring(s, 0).wait_send()
            ring(s, 1).wait_send()


def second_kernel(rows, tile, hid, tok, wd_hbm, out, wd, hb, pb, r1, rr, sn,
                  w_sem, h_sem, y_s, y_r, sib_s, sib_r, ring_s, ring_r):
    n = rows // 2
    half, width = tok.shape[0] // 2, tok.shape[1]
    piece = width // 2
    units = wd.shape[0]
    core, col, right, left, sibling, across = places(rows)
    load = pltpu.make_async_copy(wd_hbm, wd, w_sem)
    load.start()
    mine = pltpu.make_async_copy(hid, hb.at[col], h_sem)
    mine.start()
    rr[n - 1] = jnp.zeros(rr.shape[1:], BF)
    greet((right, left, sibling, across))
    mine.wait()

    def swap(s):
        return remote(hb.at[col, s], hb.at[col, s], y_s.at[s], y_r.at[s], across)

    def sib(s, d):
        return remote(pb.at[s, d, 1 - core], r1.at[s, d], sib_s.at[s, d], sib_r.at[s, d], sibling)

    def ring(s, d, k):
        return remote(sn.at[s, d, k], rr.at[s - 1, d, k], ring_s.at[s, d, k], ring_r.at[s, d, k], (left, right)[d])

    @pl.loop(0, n)
    def _(i):
        swap(n - 1 - i).start()

    load.wait()

    def product(s):
        swap(s).wait_recv()

        for k in range(2):
            @pl.loop(0, piece // tile)
            def _(t):
                start = pl.multiple_of(t * tile, tile)
                w = wd[:, pl.ds(pl.multiple_of(k * piece + t * tile, tile), tile)]
                h = jnp.concatenate([hb[0, s], hb[1, s]], axis=0)
                part = jnp.dot(h, w, preferred_element_type=F32).astype(BF)
                pb[s, :, :, k, :, pl.ds(start, tile)] = part.reshape(2, 2, half, tile)
        sib(s, 0).start()
        sib(s, 1).start()

    def added(s, d, k):
        return pb[s, d, core, k].astype(F32) + r1[s, d, k].astype(F32) + rr[s, d, k].astype(F32)

    product(n - 1)

    @pl.loop(0, n - 1)
    def _(i):
        s = n - 1 - i
        product(s - 1)
        sib(s, 0).wait_recv()
        sib(s, 1).wait_recv()
        for k in range(2):
            for d in range(2):
                @pl.when(s < n - 1)
                def _():
                    ring(s + 1, d, k).wait_recv()

                sn[s, d, k] = added(s, d, k).astype(BF)
                ring(s, d, k).start()

    sib(0, 0).wait_recv()
    sib(0, 1).wait_recv()
    for k in range(2):
        for d in range(2):
            ring(1, d, k).wait_recv()
            here = (slice(d * half, (d + 1) * half), slice(k * piece, (k + 1) * piece))
            out[here] = (tok[here].astype(F32) + added(0, d, k)).astype(BF)

    @pl.loop(0, n)
    def _(s):
        swap(s).wait_send()
        for d in range(2):
            sib(s, d).wait_send()

        @pl.when(s > 0)
        def _():
            for d in range(2):
                for k in range(2):
                    ring(s, d, k).wait_send()


def kernels(rows, cols, tokens, norm_gain, gate_proj, up_proj, down_proj):
    n = rows // 2
    count, width = tokens.shape
    half = count // 2
    units = gate_proj.shape[1]
    tile = 256 if units % 256 == 0 else 128
    vmem, hbm = pl.BlockSpec(memory_space=pltpu.VMEM), pl.BlockSpec(memory_space=pl.ANY)
    dma = pltpu.SemaphoreType.DMA
    hidden = pl.pallas_call(
        functools.partial(first_kernel, rows, cols, tile),
        out_shape=jax.ShapeDtypeStruct((n, 2 * half, units), BF),
        in_specs=[vmem, vmem, hbm, hbm],
        out_specs=vmem,
        scratch_shapes=[
            pltpu.VMEM(gate_proj.shape, BF),
            pltpu.VMEM(up_proj.shape, BF),
            pltpu.VMEM((n, 2, 2, half, width), BF),
            pltpu.VMEM((n, 2, 2, 2 * half, units), BF),
            pltpu.VMEM((n, 2, 2 * half, units), BF),
            pltpu.VMEM((count, 128), F32),
            pltpu.VMEM((count, 128), F32),
            dma((2,)), dma((2,)),
            dma((n, 2)), dma((n, 2)), dma((n, 2)), dma((n, 2)), dma((n, 2)), dma((n, 2)),
        ],
        compiler_params=pltpu.CompilerParams(
            collective_id=0, has_side_effects=True, vmem_limit_bytes=60 * 1024 * 1024
        ),
    )(tokens, norm_gain.reshape(1, width), gate_proj, up_proj)
    return pl.pallas_call(
        functools.partial(second_kernel, rows, 256),
        out_shape=jax.ShapeDtypeStruct(tokens.shape, BF),
        in_specs=[hbm, vmem, hbm],
        out_specs=vmem,
        scratch_shapes=[
            pltpu.VMEM(down_proj.shape, BF),
            pltpu.VMEM((2, n, 2 * half, units), BF),
            pltpu.VMEM((n, 2, 2, 2, half, width // 2), BF),
            pltpu.VMEM((n, 2, 2, half, width // 2), BF),
            pltpu.VMEM((n, 2, 2, half, width // 2), BF),
            pltpu.VMEM((n, 2, 2, half, width // 2), BF),
            dma, dma,
            dma((n,)), dma((n,)), dma((n, 2)), dma((n, 2)), dma((n, 2, 2)), dma((n, 2, 2)),
        ],
        compiler_params=pltpu.CompilerParams(
            collective_id=1, has_side_effects=True, vmem_limit_bytes=60 * 1024 * 1024
        ),
    )(hidden, tokens, down_proj)


def plain(rows, cols, tokens, norm_gain, gate_proj, up_proj, down_proj):
    gathered = lax.all_gather(tokens, "row", axis=0, tiled=True)
    widened = gathered.astype(jnp.float32)
    partial_squares = jnp.sum(widened * widened, axis=1)
    scaled = (widened * norm_gain.astype(jnp.float32)[None, :]).astype(jnp.bfloat16)
    gate_part = jnp.dot(scaled, gate_proj, preferred_element_type=jnp.float32)
    up_part = jnp.dot(scaled, up_proj, preferred_element_type=jnp.float32)
    gate_sum, up_sum, block_squares = (
        lax.psum_scatter(
            gate_part.astype(jnp.bfloat16), "col", scatter_dimension=0, tiled=True
        ).astype(jnp.float32),
        lax.psum_scatter(
            up_part.astype(jnp.bfloat16), "col", scatter_dimension=0, tiled=True
        ).astype(jnp.float32),
        lax.psum_scatter(
            partial_squares.astype(jnp.bfloat16), "col", scatter_dimension=0, tiled=True
        ).astype(jnp.float32),
    )
    row_scale = 1.0 / jnp.sqrt(block_squares / (tokens.shape[1] * cols) + floor_term)
    gate_value = row_scale[:, None] * gate_sum
    up_value = row_scale[:, None] * up_sum
    hidden = (jax.nn.silu(gate_value) * up_value).astype(jnp.bfloat16)
    partial_out = jnp.dot(
        lax.all_gather(hidden, "col", axis=0, tiled=True),
        down_proj,
        preferred_element_type=jnp.float32,
    )
    summed = lax.psum_scatter(
        partial_out.astype(jnp.bfloat16), "row", scatter_dimension=0, tiled=True
    ).astype(jnp.float32)
    return (tokens.astype(jnp.float32) + summed).astype(jnp.bfloat16)


def solution(mesh):
    rows, cols = mesh.shape["row"], mesh.shape["col"]
    body = kernels if cols == 2 and rows % 4 == 0 and rows >= 8 else plain
    in_specs = (P("row", "col"), P("col"), P("col", "row"), P("col", "row"), P("row", "col"))
    out_specs = P("row", "col")
    return jax.shard_map(
        functools.partial(body, rows, cols), mesh=mesh, in_specs=in_specs, out_specs=out_specs, check_vma=False
    )
```

```python
import functools

import jax
import jax.numpy as jnp
from jax import lax
from jax.experimental import pallas as pl
from jax.experimental.pallas import tpu as pltpu
from jax.sharding import PartitionSpec as P

floor_term = 0.25
MESH = pl.DeviceIdType.MESH
BF = jnp.bfloat16
F32 = jnp.float32


def places(rows):
    n = rows // 2
    row, col = lax.axis_index("row"), lax.axis_index("col")
    core, chip = row % 2, row // 2
    z, x = chip // 2, chip % 2
    pos = z + x * (n - 1 - 2 * z)

    def at(p):
        p = (p + n) % n
        far = (2 * p) // n
        return ((1 - far) * 2 * p + far * (2 * (n - 1 - p) + 1)) * 2 + core

    right, left = (at(pos + 1), col), (at(pos - 1), col)
    return core, col, right, left, (row + 1 - 2 * core, col), (row, 1 - col)


def greet(partners):
    barrier = pltpu.get_barrier_semaphore()
    for device in partners:
        pl.semaphore_signal(barrier, inc=1, device_id=device, device_id_type=MESH)
    pl.semaphore_wait(barrier, len(partners))


def remote(src, dst, send, recv, device):
    return pltpu.make_async_remote_copy(
        src_ref=src, dst_ref=dst, send_sem=send, recv_sem=recv, device_id=device, device_id_type=MESH
    )


def first_kernel(rows, cols, tile, tok, gain, wg_hbm, wu_hbm, hid, wg, wu, x, pb, rv, sq, sq_in,
                 w_sem, sq_sem, ring_s, ring_r, sib_s, sib_r, y_s, y_r):
    n = rows // 2
    half, width = tok.shape[0] // 2, tok.shape[1]
    units = wg.shape[1]
    load_g = pltpu.make_async_copy(wg_hbm, wg, w_sem.at[0])
    load_u = pltpu.make_async_copy(wu_hbm, wu, w_sem.at[1])
    load_g.start()
    load_u.start()
    core, col, right, left, sibling, across = places(rows)
    wide = tok[...].astype(F32)
    sq[...] = jnp.broadcast_to(jnp.sum(wide * wide, axis=1, keepdims=True), sq.shape)
    greet((right, left, sibling, across))
    sums = remote(sq, sq_in, sq_sem.at[0], sq_sem.at[1], across)
    sums.start()
    sums.wait()
    total = sq[:, 0:1] + sq_in[:, 0:1]
    scale = 1.0 / jnp.sqrt(total / (width * cols) + floor_term)
    normed = (tok[...].astype(F32) * gain[...].astype(F32) * scale).astype(BF)
    x[0, 0, core] = normed[:half]
    x[0, 1, core] = normed[half:]

    def ring(s, d):
        return remote(x.at[s, d, core], x.at[s + 1, d, core], ring_s.at[s, d], ring_r.at[s, d], (right, left)[d])

    def sib(s, d):
        return remote(x.at[s, d, core], x.at[s, d, core], sib_s.at[s, d], sib_r.at[s, d], sibling)

    def swap(s, g):
        return remote(pb.at[s, g, 1 - col], rv.at[s, g], y_s.at[s, g], y_r.at[s, g], across)

    def product(s, g, w):
        @pl.loop(0, units // tile)
        def _(t):
            at = pl.ds(pl.multiple_of(t * tile, tile), tile)
            part = jnp.dot(x[s].reshape(4 * half, width), w[:, at], preferred_element_type=F32)
            pb[s, g, :, :, at] = part.astype(BF).reshape(2, 2 * half, tile)
        swap(s, g).start()

    def finish(s):
        swap(s, 0).wait_recv()
        swap(s, 1).wait_recv()

        @pl.loop(0, units // tile)
        def _(t):
            at = pl.ds(pl.multiple_of(t * tile, tile), tile)
            gate = pb[s, 0, col, :, at].astype(F32) + rv[s, 0, :, at].astype(F32)
            up = pb[s, 1, col, :, at].astype(F32) + rv[s, 1, :, at].astype(F32)
            hid[s, :, at] = (gate / (1.0 + jnp.exp(-gate)) * up).astype(BF)

    def pass_on(s):
        @pl.when(s < n - 1)
        def _():
            ring(s, 0).start()
            ring(s, 1).start()

        sib(s, 0).start()
        sib(s, 1).start()

    pass_on(0)

    @pl.loop(0, n)
    def _(s):
        sib(s, 0).wait_recv()
        sib(s, 1).wait_recv()

        @pl.when(s == 0)
        def _():
            load_g.wait()

        product(s, 0, wg)

        @pl.when(s == 0)
        def _():
            load_u.wait()

        @pl.when(s < n - 1)
        def _():
            ring(s, 0).wait_recv()
            ring(s, 1).wait_recv()
            pass_on(s + 1)

        product(s, 1, wu)

        @pl.when(s > 1)
        def _():
            finish(s - 2)

    @pl.loop(n - 2, n)
    def _(s):
        finish(s)

    @pl.loop(0, n)
    def _(s):
        for d in range(2):
            sib(s, d).wait_send()
            swap(s, d).wait_send()

        @pl.when(s < n - 1)
        def _():
            ring(s, 0).wait_send()
            ring(s, 1).wait_send()


def second_kernel(rows, tile, hid, tok, wd_hbm, out, wd, hb, pb, r1, rr, sn,
                  w_sem, h_sem, y_s, y_r, sib_s, sib_r, ring_s, ring_r):
    n = rows // 2
    half, width = tok.shape[0] // 2, tok.shape[1]
    piece = width // 2
    units = wd.shape[0]
    core, col, right, left, sibling, across = places(rows)
    load = pltpu.make_async_copy(wd_hbm, wd, w_sem)
    load.start()
    mine = pltpu.make_async_copy(hid, hb.at[col], h_sem)
    mine.start()
    rr[n - 1] = jnp.zeros(rr.shape[1:], BF)
    greet((right, left, sibling, across))

    def swap(s):
        return remote(hid.at[s], hb.at[col, s], y_s.at[s], y_r.at[s], across)

    def sib(s, d, k):
        return remote(pb.at[s, d, 1 - core, k], r1.at[s, d, k], sib_s.at[s, d, k], sib_r.at[s, d, k], sibling)

    def ring(s, d, k):
        return remote(sn.at[s, d, k], rr.at[s - 1, d, k], ring_s.at[s, d, k], ring_r.at[s, d, k], (left, right)[d])

    @pl.loop(0, n)
    def _(i):
        swap(n - 1 - i).start()

    mine.wait()
    load.wait()

    def product(s, k):
        @pl.loop(0, piece // tile)
        def _(t):
            start = pl.multiple_of(t * tile, tile)
            w = wd[:, pl.ds(pl.multiple_of(k * piece + t * tile, tile), tile)]
            h = jnp.concatenate([hb[0, s], hb[1, s]], axis=0)
            part = jnp.dot(h, w, preferred_element_type=F32).astype(BF)
            pb[s, :, :, k, :, pl.ds(start, tile)] = part.reshape(2, 2, half, tile)
        sib(s, 0, k).start()
        sib(s, 1, k).start()

    def added(s, d, k):
        return pb[s, d, core, k].astype(F32) + r1[s, d, k].astype(F32) + rr[s, d, k].astype(F32)

    def stage(s, k):
        for d in range(2):
            sib(s, d, k).wait_recv()

            @pl.when(s < n - 1)
            def _():
                ring(s + 1, d, k).wait_recv()

            sn[s, d, k] = added(s, d, k).astype(BF)
            ring(s, d, k).start()

    @pl.loop(0, n)
    def _(i):
        s = n - 1 - i
        swap(s).wait_recv()
        product(s, 0)

        @pl.when(i > 0)
        def _():
            stage(s + 1, 1)

        product(s, 1)

        @pl.when(s > 0)
        def _():
            stage(s, 0)

    for k in range(2):
        for d in range(2):
            sib(0, d, k).wait_recv()
            ring(1, d, k).wait_recv()
            here = (slice(d * half, (d + 1) * half), slice(k * piece, (k + 1) * piece))
            out[here] = (tok[here].astype(F32) + added(0, d, k)).astype(BF)

    @pl.loop(0, n)
    def _(s):
        swap(s).wait_send()
        for d in range(2):
            for k in range(2):
                sib(s, d, k).wait_send()

        @pl.when(s > 0)
        def _():
            for d in range(2):
                for k in range(2):
                    ring(s, d, k).wait_send()


def kernels(rows, cols, tokens, norm_gain, gate_proj, up_proj, down_proj):
    n = rows // 2
    count, width = tokens.shape
    half = count // 2
    units = gate_proj.shape[1]
    tile = 256 if units % 256 == 0 else 128
    vmem, hbm = pl.BlockSpec(memory_space=pltpu.VMEM), pl.BlockSpec(memory_space=pl.ANY)
    dma = pltpu.SemaphoreType.DMA
    hidden = pl.pallas_call(
        functools.partial(first_kernel, rows, cols, tile),
        out_shape=jax.ShapeDtypeStruct((n, 2 * half, units), BF),
        in_specs=[vmem, vmem, hbm, hbm],
        out_specs=vmem,
        scratch_shapes=[
            pltpu.VMEM(gate_proj.shape, BF),
            pltpu.VMEM(up_proj.shape, BF),
            pltpu.VMEM((n, 2, 2, half, width), BF),
            pltpu.VMEM((n, 2, 2, 2 * half, units), BF),
            pltpu.VMEM((n, 2, 2 * half, units), BF),
            pltpu.VMEM((count, 128), F32),
            pltpu.VMEM((count, 128), F32),
            dma((2,)), dma((2,)),
            dma((n, 2)), dma((n, 2)), dma((n, 2)), dma((n, 2)), dma((n, 2)), dma((n, 2)),
        ],
        compiler_params=pltpu.CompilerParams(
            collective_id=0, has_side_effects=True, vmem_limit_bytes=60 * 1024 * 1024
        ),
    )(tokens, norm_gain.reshape(1, width), gate_proj, up_proj)
    return pl.pallas_call(
        functools.partial(second_kernel, rows, 256),
        out_shape=jax.ShapeDtypeStruct(tokens.shape, BF),
        in_specs=[hbm, vmem, hbm],
        out_specs=vmem,
        scratch_shapes=[
            pltpu.VMEM(down_proj.shape, BF),
            pltpu.VMEM((2, n, 2 * half, units), BF),
            pltpu.VMEM((n, 2, 2, 2, half, width // 2), BF),
            pltpu.VMEM((n, 2, 2, half, width // 2), BF),
            pltpu.VMEM((n, 2, 2, half, width // 2), BF),
            pltpu.VMEM((n, 2, 2, half, width // 2), BF),
            dma, dma,
            dma((n,)), dma((n,)), dma((n, 2, 2)), dma((n, 2, 2)), dma((n, 2, 2)), dma((n, 2, 2)),
        ],
        compiler_params=pltpu.CompilerParams(
            collective_id=1, has_side_effects=True, vmem_limit_bytes=60 * 1024 * 1024
        ),
    )(hidden, tokens, down_proj)


def plain(rows, cols, tokens, norm_gain, gate_proj, up_proj, down_proj):
    gathered = lax.all_gather(tokens, "row", axis=0, tiled=True)
    widened = gathered.astype(jnp.float32)
    partial_squares = jnp.sum(widened * widened, axis=1)
    scaled = (widened * norm_gain.astype(jnp.float32)[None, :]).astype(jnp.bfloat16)
    gate_part = jnp.dot(scaled, gate_proj, preferred_element_type=jnp.float32)
    up_part = jnp.dot(scaled, up_proj, preferred_element_type=jnp.float32)
    gate_sum, up_sum, block_squares = (
        lax.psum_scatter(
            gate_part.astype(jnp.bfloat16), "col", scatter_dimension=0, tiled=True
        ).astype(jnp.float32),
        lax.psum_scatter(
            up_part.astype(jnp.bfloat16), "col", scatter_dimension=0, tiled=True
        ).astype(jnp.float32),
        lax.psum_scatter(
            partial_squares.astype(jnp.bfloat16), "col", scatter_dimension=0, tiled=True
        ).astype(jnp.float32),
    )
    row_scale = 1.0 / jnp.sqrt(block_squares / (tokens.shape[1] * cols) + floor_term)
    gate_value = row_scale[:, None] * gate_sum
    up_value = row_scale[:, None] * up_sum
    hidden = (jax.nn.silu(gate_value) * up_value).astype(jnp.bfloat16)
    partial_out = jnp.dot(
        lax.all_gather(hidden, "col", axis=0, tiled=True),
        down_proj,
        preferred_element_type=jnp.float32,
    )
    summed = lax.psum_scatter(
        partial_out.astype(jnp.bfloat16), "row", scatter_dimension=0, tiled=True
    ).astype(jnp.float32)
    return (tokens.astype(jnp.float32) + summed).astype(jnp.bfloat16)


def solution(mesh):
    rows, cols = mesh.shape["row"], mesh.shape["col"]
    body = kernels if cols == 2 and rows % 4 == 0 and rows >= 8 else plain
    in_specs = (P("row", "col"), P("col"), P("col", "row"), P("col", "row"), P("row", "col"))
    out_specs = P("row", "col")
    return jax.shard_map(
        functools.partial(body, rows, cols), mesh=mesh, in_specs=in_specs, out_specs=out_specs, check_vma=False
    )
```
